32 devices in a mesh: rows: 16 (over z, y, x), cols: 2 (over core).
Axes of the slice: x: 2, y: 2, z: 4, core: 2. Of those that a mesh axis runs over, the one named last changes fastest.
Arguments:
- rhs: float32 [2, 96, 6144], P('cols', 'rows'), may hold values from -6 to 6
- pattern: int32 [48, 2], P(None, 'cols'), may hold values 0 or 1
- front_blocks: int32 [16, 4], replicated, may hold values from 0 to 47, as said below
- front_slot: int32 [16], replicated, may hold values from 0 to 31, as said below
- pivot_inverse: float32 [32, 256, 256], P('rows'), may hold values from -0.375 to 0.375
- update_factor: float32 [32, 256, 256], P('rows'), may hold values from -0.375 to 0.375
Outputs:
- solution: float32 [2, 96, 6144], P('cols', 'rows')
The draws below stay inside these ranges and needn't reach their ends.
Inputs may be any that keep to these rules, and one draw needn't show every extreme that they name: `front_blocks`: columns 0 and 1 together name every row block that is no contribution block exactly once; columns 2 and 3 of a front are two different blocks, never a pivot block of any front. `front_slot`: all different; slot s belongs to index s // 2 of rows; some index holds 2 fronts in every draw; slots that no front names are unused.
All inputs are finite; a program needn't handle non-finite values. No bound on the sum of `pattern` on one device may be relied on, other than what follows from the above.
Results may differ from the reference program's by a relative error of at most 0.0001.
Values sent between devices are 32-bit elements; how exact they have to be, the bound alone decides.
A program may use at most 64 MiB of HBM per device.

```python
import jax
import jax.numpy as jnp
from jax import lax

BLOCK = 128
PIV = 256
SLOT_DEV = 2
FRONTS = 16
SLOTS = 32
RB = 48
NROWS = 6144
GROUPS = 2
GCOLS = 96


def draw_front_blocks(key, part):
    shuffled = jax.random.permutation(jax.random.fold_in(key, 11), RB).astype(jnp.int32)
    pivots = shuffled[:2 * FRONTS].reshape(FRONTS, 2)
    separators = shuffled[2 * FRONTS:]
    first_sep = jax.random.randint(jax.random.fold_in(key, 12), (FRONTS,), 0, FRONTS).astype(jnp.int32)
    stride_draw = jax.random.randint(jax.random.fold_in(key, 13), (FRONTS,), 1, FRONTS).astype(jnp.int32)
    second_sep = (first_sep + stride_draw) % FRONTS
    return jnp.concatenate([pivots, separators[first_sep][:, None], separators[second_sep][:, None]], axis=1).astype(jnp.int32)


def draw_front_slot(key, part):
    shuffled = jax.random.permutation(jax.random.fold_in(key, 21), SLOTS).astype(jnp.int32)
    chosen = shuffled[:FRONTS]
    leading = chosen[0]
    partner = leading - leading % SLOT_DEV + (leading % SLOT_DEV + 1) % SLOT_DEV
    displaced = chosen[1]
    chosen = jnp.where(chosen == partner, displaced, chosen)
    chosen = chosen.at[1].set(partner)
    return chosen.astype(jnp.int32)


def set_ends(entries, rng, low, largest):
    extent = entries.shape
    place = [jax.random.randint(jax.random.fold_in(rng, axis), (), 0, extent[axis]) for axis in range(len(extent))]
    entries = entries.at[tuple(place)].set(low)
    longest = extent.index(max(extent))
    place[longest] = (place[longest] + 1) % extent[longest]
    return entries.at[tuple(place)].set(largest)


def steps_of(stream_key, extent, pieces, smallest, high):
    def one(dim, shards_of):
        steps = jax.random.uniform(jax.random.fold_in(jax.random.fold_in(stream_key, 6), dim), (shards_of,), jnp.float32, smallest / len(pieces), high / len(pieces))
        return jnp.repeat(jnp.exp(steps), extent[dim] // shards_of).reshape((-1,) + (1,) * (len(extent) - dim - 1))

    factor_of = one(*pieces[0])
    for cut in pieces[1:]:
        factor_of = factor_of * one(*cut)
    return factor_of


def centred(stream_key, shape, width, reach, pieces=(), kind=jnp.bfloat16):
    factor_of = steps_of(stream_key, shape, pieces, -0.22, 0.18) if pieces else 1.0
    array = jax.random.normal(stream_key, shape, jnp.float32) * width * factor_of
    return jnp.minimum(jnp.maximum(array, -reach), reach).astype(kind)


def setup_inputs(seed: int = 0) -> dict:
    seeds = jax.random.split(jax.random.key(seed), 7)
    return {
        "rhs": centred(seeds[0], (GROUPS, GCOLS, NROWS), 1.0, 6.0, ((0, 2), (1, 16)), jnp.float32),
        "pattern": set_ends((jax.random.randint(seeds[1], (RB, GROUPS), 0, 4) < 3).astype(jnp.int32), jax.random.fold_in(seeds[1], 1), 0, 1),
        "front_blocks": draw_front_blocks(jax.random.fold_in(seeds[6], 71), 0),
        "front_slot": draw_front_slot(jax.random.fold_in(seeds[6], 71), 0),
        "pivot_inverse": centred(seeds[4], (SLOTS, PIV, PIV), PIV ** -0.5, 0.375, ((0, 16),), jnp.float32),
        "update_factor": centred(seeds[5], (SLOTS, PIV, PIV), PIV ** -0.5, 0.375, ((0, 16),), jnp.float32),
    }


def reference(rhs, pattern, front_blocks, front_slot, pivot_inverse, update_factor):
    offsets = jnp.arange(BLOCK, dtype=jnp.int32)
    rows_of = (front_blocks[:, :, None] * BLOCK + offsets[None, None, :]).reshape(FRONTS, 4 * BLOCK).astype(jnp.int32)
    row_mask = jnp.repeat(pattern.astype(jnp.float32), BLOCK, axis=0)
    masked = rhs * jnp.transpose(row_mask)[:, None, :]
    strict_lower = jnp.tril(jnp.ones((PIV, PIV), jnp.float32), -1)
    identity = jnp.eye(PIV, dtype=jnp.float32)

    def one_front(result, front_index):
        rows = rows_of[front_index]
        slot_index = front_slot[front_index]
        pivots = jnp.take(masked, rows[:PIV], axis=2)
        inverse = identity + strict_lower * pivot_inverse[slot_index]
        solved = jnp.einsum("gcj,ij->gci", pivots, inverse, precision=lax.Precision.HIGHEST)
        update = jnp.einsum("gcj,ij->gci", solved, update_factor[slot_index], precision=lax.Precision.HIGHEST)
        result = result.at[:, :, rows[:PIV]].set(solved)
        result = result.at[:, :, rows[PIV:]].add(-update)
        return result, None

    result, _ = lax.scan(one_front, masked, jnp.arange(FRONTS, dtype=jnp.int32))
    return result
```

```python
import functools

import jax
import jax.numpy as jnp
from jax import lax
from jax.experimental import pallas as pl
from jax.experimental.pallas import tpu as pltpu
from jax.sharding import PartitionSpec as P

BLOCK = 128
COLS = 6
PAIR = 2


def split(value):
    high = value.astype(jnp.bfloat16)
    low = (value - high.astype(jnp.float32)).astype(jnp.bfloat16)
    return high, low


def times_transposed(x, high, low):
    dims = (((1,), (1,)), ((), ()))
    x_high, x_low = split(x)
    dot = functools.partial(lax.dot_general, dimension_numbers=dims, preferred_element_type=jnp.float32)
    return dot(x_high, high) + (dot(x_low, high) + dot(x_high, low))


def kernel(
    n, fronts, blocks,
    rhs_hbm, pattern_hbm, fb_hbm, slot_hbm, inv_hbm, upd_hbm,
    out_ref,
    x, snd, rcv, back, pool, last, fourth, inv, upd, wide, coef,
    pattern, fb, slot, front_of, src, sep,
    local_sem, out_send, out_recv, back_send, back_recv,
):
    me = lax.axis_index("rows")
    col = lax.axis_index("cols")
    slots = PAIR * n
    seps = blocks - 2 * fronts

    def target(peer):
        return {"rows": peer, "cols": col}

    pieces = [
        (rhs_hbm, x), (pattern_hbm, pattern), (fb_hbm, fb), (slot_hbm, slot), (inv_hbm, inv), (upd_hbm, upd),
    ]
    loads = [pltpu.make_async_copy(a, b, local_sem.at[i]) for i, (a, b) in enumerate(pieces)]
    for load in (loads[1], loads[2], loads[3], loads[0], loads[4], loads[5]):
        load.start()

    barrier = pltpu.get_barrier_semaphore()

    def greet(i, carry):
        pl.semaphore_signal(
            barrier, inc=1, device_id=target(lax.rem(me + i, n)), device_id_type=pl.DeviceIdType.MESH
        )
        return carry

    lax.fori_loop(1, n, greet, 0)

    few = fronts <= 16

    def total(count, term):
        if few:
            values = [term(i) for i in range(count)]
            while len(values) > 1:
                pairs = [a + b for a, b in zip(values[::2], values[1::2])]
                values = pairs + ([values[-1]] if len(values) % 2 else [])
            return values[0]
        return lax.fori_loop(0, count, lambda i, t: t + term(i), 0)

    for load in loads[1:4]:
        load.wait()

    def find_front(s, carry):
        front_of[s] = jnp.minimum(total(fronts, lambda f: jnp.where(slot[f] == s, f, 0)), fronts - 1)
        return carry

    lax.fori_loop(0, slots, find_front, 0)
    loads[0].wait()

    def block_rows(b, first, count):
        mask = pattern[b].astype(jnp.float32)
        return x[pl.ds(first * blocks + b, count, stride=blocks), :] * mask

    def pack(d, carry):
        f0 = front_of[PAIR * d]
        f1 = front_of[PAIR * d + 1]
        snd[d, 0, 0:6, :] = block_rows(fb[0, f0], 0, COLS)
        snd[d, 1, 0:6, :] = block_rows(fb[1, f0], 0, COLS)
        snd[d, 2, 0:6, :] = block_rows(fb[0, f1], 0, COLS)
        b3 = fb[1, f1]
        for t in range(3):
            snd[d, t, 6:8, :] = block_rows(b3, 2 * t, 2)
        return carry

    lax.fori_loop(0, n, pack, 0)
    pl.semaphore_wait(barrier, n - 1)

    order = sorted(range(1, n), key=lambda i: abs(i - n // 2))
    runs = order if n <= 16 else None

    def for_peers(body):
        if runs is not None:
            for i in runs:
                body(lax.rem(me + i, n))
        else:
            def step(i, carry):
                body(lax.rem(me + i, n))
                return carry
            lax.fori_loop(1, n, step, 0)

    def send_out(peer):
        pltpu.make_async_remote_copy(
            src_ref=snd.at[peer], dst_ref=rcv.at[me], send_sem=out_send, recv_sem=out_recv,
            device_id=target(peer), device_id_type=pl.DeviceIdType.MESH,
        ).start()

    for_peers(send_out)
    rcv[pl.ds(me, 1)] = snd[pl.ds(me, 1)]

    loads[4].wait()
    loads[5].wait()
    width = inv.shape[1]
    strict = lax.broadcasted_iota(jnp.int32, (width, width), 0) > lax.broadcasted_iota(jnp.int32, (width, width), 1)
    for k in range(PAIR):
        wide[k, 0], wide[k, 1] = split(jnp.where(strict, inv[k], 0.0))
        wide[k, 2], wide[k, 3] = split(upd[k])

    def find_source(b, rank):
        def term(e):
            h, f = e // fronts, e % fronts
            return jnp.where(fb[h, f] == b, 3 * slot[f] + h + 1, 0)

        place = total(2 * fronts, term)
        is_sep = place == 0
        src[b] = jnp.minimum(jnp.where(is_sep, 3 * slots + rank, place - 1), 3 * slots + seps - 1)
        return rank + jnp.where(is_sep, 1, 0)

    lax.fori_loop(0, blocks, find_source, 0)

    def find_separator(j, carry):
        def step(b, t):
            return t + jnp.where(src[b] == 3 * slots + j, b, 0)
        b = lax.fori_loop(0, blocks, step, 0, unroll=8)
        b = jnp.minimum(b, blocks - 1)
        sep[j] = b

        def weight(e, c):
            h, f = e // fronts, e % fronts
            hit = jnp.where(fb[2 + h, f] == b, -1.0, 0.0).astype(jnp.float32)
            coef[pl.ds(j * 2 * fronts + e, 1), :] = jnp.full((1, BLOCK), hit, jnp.float32)
            return c
        lax.fori_loop(0, 2 * fronts, weight, 0, unroll=8)
        return carry

    lax.fori_loop(0, seps, find_separator, 0)

    def landed(buffer, count, sem):
        view = buffer.at[pl.ds(0, count)]
        return pltpu.make_async_copy(view, view, sem)

    landed(rcv, n - 1, out_recv).wait()

    fourth[:, 6:8, :] = jnp.zeros((n, 2, BLOCK), jnp.float32)
    for t in range(3):
        fourth[:, 2 * t:2 * t + 2, :] = rcv[:, t, 6:8, :]

    def flat(a):
        return a.reshape(8 * n, BLOCK)

    for k in range(PAIR):
        if k == 0:
            pivots = jnp.concatenate([flat(rcv[:, 0]), flat(rcv[:, 1])], axis=1)
        else:
            pivots = jnp.concatenate([flat(rcv[:, 2]), flat(fourth[...])], axis=1)
        solved = pivots + times_transposed(pivots, wide[k, 0], wide[k, 1])
        update = times_transposed(solved, wide[k, 2], wide[k, 3])
        quads = [
            half.reshape(n, 8, BLOCK)
            for half in (solved[:, :BLOCK], solved[:, BLOCK:], update[:, :BLOCK], update[:, BLOCK:])
        ]
        for t in range(3):
            back[k, :, t, 0:6, :] = quads[t][:, 0:6]
            back[k, :, t, 6:8, :] = quads[3][:, 2 * t:2 * t + 2]

        def send_back(peer, k=k):
            pltpu.make_async_remote_copy(
                src_ref=back.at[k, peer], dst_ref=pool.at[pl.ds(3 * (PAIR * me + k), 3)],
                send_sem=back_send, recv_sem=back_recv,
                device_id=target(peer), device_id_type=pl.DeviceIdType.MESH,
            ).start()

        for_peers(send_back)
        pool[pl.ds(3 * (PAIR * me + k), 3)] = back[k, me]

    landed(pool, 3 * PAIR * (n - 1), back_recv).wait()

    for t in range(3):
        last[:, 2 * t:2 * t + 2, :] = pool[pl.ds(t, slots, stride=3), 6:8, :]

    def add_up(j, carry):
        b = sep[j]
        acc = block_rows(b, 0, COLS)

        def term_first(f, a):
            return a + coef[pl.ds(j * 2 * fronts + f, 1), :] * pool[3 * slot[f] + 2, 0:6, :]

        def term_second(f, a):
            return a + coef[pl.ds(j * 2 * fronts + fronts + f, 1), :] * last[slot[f]]
        acc = lax.fori_loop(0, fronts, term_first, acc, unroll=8)
        acc = lax.fori_loop(0, fronts, term_second, acc, unroll=8)
        pool[3 * slots + j, 0:6, :] = acc
        return carry

    lax.fori_loop(0, seps, add_up, 0)

    def place(b, carry):
        out_ref[pl.ds(b, COLS, stride=blocks), :] = pool[src[b], 0:6, :]
        return carry

    lax.fori_loop(0, blocks, place, 0, unroll=8)

    landed(snd, n - 1, out_send).wait()
    for k in range(PAIR):
        landed(back.at[k], n - 1, back_send).wait()


def on_device(n, rhs, pattern, front_blocks, front_slot, pivot_inverse, update_factor):
    fronts = front_blocks.shape[0]
    columns, total_rows = rhs.shape[1:]
    blocks = total_rows // BLOCK
    assert columns == COLS and pivot_inverse.shape[0] == PAIR
    width = pivot_inverse.shape[1]
    slots = PAIR * n
    seps = blocks - 2 * fronts
    f32, i32 = jnp.float32, jnp.int32
    result = pl.pallas_call(
        functools.partial(kernel, n, fronts, blocks),
        out_shape=jax.ShapeDtypeStruct((columns * blocks, BLOCK), f32),
        in_specs=[pl.BlockSpec(memory_space=pl.ANY)] * 6,
        out_specs=pl.BlockSpec(memory_space=pltpu.VMEM),
        scratch_shapes=[
            pltpu.VMEM((columns * blocks, BLOCK), f32),
            pltpu.VMEM((n, 3, 8, BLOCK), f32),
            pltpu.VMEM((n, 3, 8, BLOCK), f32),
            pltpu.VMEM((PAIR, n, 3, 8, BLOCK), f32),
            pltpu.VMEM((3 * slots + seps, 8, BLOCK), f32),
            pltpu.VMEM((slots, 6, BLOCK), f32),
            pltpu.VMEM((n, 8, BLOCK), f32),
            pltpu.VMEM((PAIR, width, width), f32),
            pltpu.VMEM((PAIR, width, width), f32),
            pltpu.VMEM((PAIR, 4, width, width), jnp.bfloat16),
            pltpu.VMEM((seps * 2 * fronts, BLOCK), f32),
            pltpu.SMEM((blocks,), i32),
            pltpu.SMEM((4, fronts), i32),
            pltpu.SMEM((fronts,), i32),
            pltpu.SMEM((slots,), i32),
            pltpu.SMEM((blocks,), i32),
            pltpu.SMEM((seps,), i32),
            pltpu.SemaphoreType.DMA((6,)),
            pltpu.SemaphoreType.DMA,
            pltpu.SemaphoreType.DMA,
            pltpu.SemaphoreType.DMA,
            pltpu.SemaphoreType.DMA,
        ],
        compiler_params=pltpu.CompilerParams(collective_id=0, has_side_effects=True),
    )(
        rhs.reshape(columns * blocks, BLOCK),
        pattern.reshape(-1),
        front_blocks.T,
        front_slot,
        pivot_inverse,
        update_factor,
    )
    return result.reshape(1, columns, total_rows)


def solution(mesh):
    return jax.shard_map(
        functools.partial(on_device, mesh.shape["rows"]),
        mesh=mesh,
        in_specs=(
            P("cols", "rows", None),
            P(None, "cols"),
            P(),
            P(),
            P("rows", None, None),
            P("rows", None, None),
        ),
        out_specs=P("cols", "rows", None),
        check_vma=False,
    )
```

```python
import functools

import jax
import jax.numpy as jnp
from jax import lax
from jax.experimental import pallas as pl
from jax.experimental.pallas import tpu as pltpu
from jax.sharding import PartitionSpec as P

BLOCK = 128
COLS = 6
PAIR = 2


def split(value):
    high = value.astype(jnp.bfloat16)
    low = (value - high.astype(jnp.float32)).astype(jnp.bfloat16)
    return high, low


def times_transposed(x, high, low):
    dims = (((1,), (1,)), ((), ()))
    x_high, x_low = split(x)
    dot = functools.partial(lax.dot_general, dimension_numbers=dims, preferred_element_type=jnp.float32)
    return dot(x_high, high) + (dot(x_low, high) + dot(x_high, low))


def kernel(
    n, fronts, blocks, chunk,
    rhs_hbm, pattern_hbm, fb_hbm, slot_hbm, inv_hbm, upd_hbm,
    out_ref,
    x, snd, rcv, back, pool, last, halves, inv, upd, wide, sep_rows, coef,
    pattern, fb, slot, front_of, place_of, src, sep,
    local_sem, out_send, out_recv, back_send, back_recv,
):
    me = lax.axis_index("rows")
    col = lax.axis_index("cols")
    slots = PAIR * n
    seps = blocks - 2 * fronts
    few = n <= 16

    def target(peer):
        return {"rows": peer, "cols": col}

    order = sorted(range(1, n), key=lambda i: abs(i - n // 2))

    def for_peers(body):
        if few:
            for i in order:
                body(lax.rem(me + i, n))
        else:
            def step(i, carry):
                body(lax.rem(me + i, n))
                return carry
            lax.fori_loop(1, n, step, 0)

    def repeat(count, body, unroll=1):
        def step(i, carry):
            body(i)
            return carry
        lax.fori_loop(0, count, step, 0, unroll=unroll if few else 1)

    pieces = [
        (rhs_hbm, x), (pattern_hbm, pattern), (fb_hbm, fb), (slot_hbm, slot), (inv_hbm, inv), (upd_hbm, upd),
    ]
    loads = [pltpu.make_async_copy(a, b, local_sem.at[i]) for i, (a, b) in enumerate(pieces)]
    for i in (3, 2, 1, 0, 4, 5):
        loads[i].start()

    barrier = pltpu.get_barrier_semaphore()
    for_peers(lambda peer: pl.semaphore_signal(
        barrier, inc=1, device_id=target(peer), device_id_type=pl.DeviceIdType.MESH
    ))

    def total(count, term):
        if few:
            values = [term(i) for i in range(count)]
            while len(values) > 1:
                pairs = [a + b for a, b in zip(values[::2], values[1::2])]
                values = pairs + ([values[-1]] if len(values) % 2 else [])
            return values[0]
        return lax.fori_loop(0, count, lambda i, t: t + term(i), 0)

    loads[3].wait()

    def find_front(s):
        front_of[s] = jnp.minimum(total(fronts, lambda f: jnp.where(slot[f] == s, f, 0)), fronts - 1)

    repeat(slots, find_front, 2)
    for i in (2, 1, 0):
        loads[i].wait()

    def block_rows(b, first, count):
        mask = pattern[b].astype(jnp.float32)
        return x[pl.ds(first * blocks + b, count, stride=blocks), :] * mask

    def pack(d):
        for k in range(PAIR):
            f = front_of[PAIR * d + k]
            b0, b1 = fb[0, f], fb[1, f]
            snd[k, d, 0] = block_rows(b0, 0, 4)
            snd[k, d, 1, 0:2, :] = block_rows(b0, 4, 2)
            snd[k, d, 1, 2:4, :] = block_rows(b1, 0, 2)
            snd[k, d, 2] = block_rows(b1, 2, 4)

    repeat(n, pack, 2)
    pl.semaphore_wait(barrier, n - 1)

    for k in range(PAIR):
        for_peers(lambda peer, k=k: pltpu.make_async_remote_copy(
            src_ref=snd.at[k, peer], dst_ref=rcv.at[k, me], send_sem=out_send.at[k], recv_sem=out_recv.at[k],
            device_id=target(peer), device_id_type=pl.DeviceIdType.MESH,
        ).start())
        rcv[k, me] = snd[k, me]

    loads[4].wait()
    loads[5].wait()
    width = inv.shape[1]
    strict = lax.broadcasted_iota(jnp.int32, (width, width), 0) > lax.broadcasted_iota(jnp.int32, (width, width), 1)
    for k in range(PAIR):
        wide[k, 0], wide[k, 1] = split(jnp.where(strict, inv[k], 0.0))
        wide[k, 2], wide[k, 3] = split(upd[k])
    halves[...] = jnp.zeros(halves.shape, jnp.float32)
    last[...] = jnp.zeros(last.shape, jnp.float32)

    def find_place(f):
        s = slot[f]
        place_of[f] = 3 * (lax.rem(s, PAIR) * n + lax.div(s, PAIR)) + 1

    repeat(fronts, find_place, 4)

    def find_source(b, rank):
        def term(f):
            at = place_of[f]
            return jnp.where(fb[0, f] == b, at, 0) + jnp.where(fb[1, f] == b, at + 1, 0)

        place = total(fronts, term)
        is_sep = place == 0
        src[b] = jnp.minimum(jnp.where(is_sep, 3 * slots + rank, place - 1), 3 * slots + seps - 1)
        return rank + jnp.where(is_sep, 1, 0)

    lax.fori_loop(0, blocks, find_source, 0)

    def landed(buffer, count, sem):
        view = buffer.at[pl.ds(0, count)]
        return pltpu.make_async_copy(view, view, sem)

    def flat(a):
        return a.reshape(8 * n, BLOCK)

    for k in range(PAIR):
        landed(rcv.at[k], n - 1, out_recv.at[k]).wait()
        halves[0, :, 0:4, :] = rcv[k, :, 0]
        halves[0, :, 4:6, :] = rcv[k, :, 1, 0:2, :]
        halves[1, :, 0:2, :] = rcv[k, :, 1, 2:4, :]
        halves[1, :, 2:6, :] = rcv[k, :, 2]
        pivots = jnp.concatenate([flat(halves[0]), flat(halves[1])], axis=1)
        solved = pivots + times_transposed(pivots, wide[k, 0], wide[k, 1])
        update = times_transposed(solved, wide[k, 2], wide[k, 3])
        quads = [
            half.reshape(n, 8, BLOCK)
            for half in (solved[:, :BLOCK], solved[:, BLOCK:], update[:, :BLOCK], update[:, BLOCK:])
        ]
        for t in range(3):
            back[k, :, t, 0:6, :] = quads[t][:, 0:6]
            back[k, :, t, 6:8, :] = quads[3][:, 2 * t:2 * t + 2]

        for_peers(lambda peer, k=k: pltpu.make_async_remote_copy(
            src_ref=back.at[k, peer], dst_ref=pool.at[pl.ds(3 * (k * n + me), 3)],
            send_sem=back_send.at[k], recv_sem=back_recv.at[k],
            device_id=target(peer), device_id_type=pl.DeviceIdType.MESH,
        ).start())
        pool[pl.ds(3 * (k * n + me), 3)] = back[k, me]

    def find_separator(j):
        b = lax.fori_loop(
            0, blocks, lambda b, t: t + jnp.where(src[b] == 3 * slots + j, b, 0), 0, unroll=16 if few else 1
        )
        b = jnp.minimum(b, blocks - 1)
        sep[j] = b
        sep_rows[pl.ds(j, 1), :] = jnp.full((1, BLOCK), b, jnp.int32)
        pool[3 * slots + j, 0:6, :] = block_rows(b, 0, COLS)
        pool[3 * slots + j, 6:8, :] = jnp.zeros((2, BLOCK), jnp.float32)

    repeat(seps, find_separator)

    def weigh(g):
        rows = sep_rows[pl.ds(pl.multiple_of(g * chunk, chunk), chunk), :]

        def one_slot(s):
            f = front_of[s]
            used = slot[f] == s
            q = lax.rem(s, PAIR) * n + lax.div(s, PAIR)
            for h in range(2):
                named = jnp.where(used, fb[2 + h, f], -1)
                coef[(g * slots + q) * 2 + h] = jnp.where(rows == named, -1.0, 0.0)

        repeat(slots, one_slot, 4)

    repeat(seps // chunk, weigh)

    for k in range(PAIR):
        landed(pool, 3 * (n - 1), back_recv.at[k]).wait()
        for t in range(3):
            last[k * n:(k + 1) * n, 2 * t:2 * t + 2, :] = pool[pl.ds(3 * k * n + t, n, stride=3), 6:8, :]

        def add_up(g, k=k):
            first = 3 * slots + g * chunk

            def one_slot(o, accs):
                q = k * n + o
                parts = (pool[3 * q + 2], last[q])
                for h in range(2):
                    row = (g * slots + q) * 2 + h
                    accs = tuple(a + coef[row, j:j + 1, :] * parts[h] for j, a in enumerate(accs))
                return accs

            accs = tuple(pool[first + j] for j in range(chunk))
            accs = lax.fori_loop(0, n, one_slot, accs, unroll=4 if few else 1)
            for j in range(chunk):
                pool[first + j] = accs[j]

        repeat(seps // chunk, add_up)

    def put(b):
        out_ref[pl.ds(b, COLS, stride=blocks), :] = pool[src[b], 0:6, :]

    repeat(blocks, put, 16)

    for k in range(PAIR):
        landed(snd.at[k], n - 1, out_send.at[k]).wait()
        landed(back.at[k], n - 1, back_send.at[k]).wait()


def on_device(n, rhs, pattern, front_blocks, front_slot, pivot_inverse, update_factor):
    fronts = front_blocks.shape[0]
    columns, total_rows = rhs.shape[1:]
    blocks = total_rows // BLOCK
    assert columns == COLS and pivot_inverse.shape[0] == PAIR
    width = pivot_inverse.shape[1]
    slots = PAIR * n
    seps = blocks - 2 * fronts
    f32, i32 = jnp.float32, jnp.int32
    chunk = next(c for c in (16, 8, 4, 2, 1) if seps % c == 0)
    result = pl.pallas_call(
        functools.partial(kernel, n, fronts, blocks, chunk),
        out_shape=pltpu.VMEM((columns * blocks, BLOCK), f32),
        in_specs=[pl.BlockSpec(memory_space=pl.ANY)] * 6,
        out_specs=pl.BlockSpec(memory_space=pltpu.VMEM),
        scratch_shapes=[
            pltpu.VMEM((columns * blocks, BLOCK), f32),
            pltpu.VMEM((PAIR, n, 3, 4, BLOCK), f32),
            pltpu.VMEM((PAIR, n, 3, 4, BLOCK), f32),
            pltpu.VMEM((PAIR, n, 3, 8, BLOCK), f32),
            pltpu.VMEM((3 * slots + seps, 8, BLOCK), f32),
            pltpu.VMEM((slots, 8, BLOCK), f32),
            pltpu.VMEM((2, n, 8, BLOCK), f32),
            pltpu.VMEM((PAIR, width, width), f32),
            pltpu.VMEM((PAIR, width, width), f32),
            pltpu.VMEM((PAIR, 4, width, width), jnp.bfloat16),
            pltpu.VMEM((seps, BLOCK), i32),
            pltpu.VMEM((seps // chunk * slots * 2, chunk, BLOCK), f32),
            pltpu.SMEM((blocks,), i32),
            pltpu.SMEM((4, fronts), i32),
            pltpu.SMEM((fronts,), i32),
            pltpu.SMEM((slots,), i32),
            pltpu.SMEM((fronts,), i32),
            pltpu.SMEM((blocks,), i32),
            pltpu.SMEM((seps,), i32),
            pltpu.SemaphoreType.DMA((6,)),
            pltpu.SemaphoreType.DMA((PAIR,)),
            pltpu.SemaphoreType.DMA((PAIR,)),
            pltpu.SemaphoreType.DMA((PAIR,)),
            pltpu.SemaphoreType.DMA((PAIR,)),
        ],
        compiler_params=pltpu.CompilerParams(collective_id=0, has_side_effects=True),
    )(
        rhs.reshape(columns * blocks, BLOCK),
        pattern.reshape(-1),
        front_blocks.T,
        front_slot,
        pivot_inverse,
        update_factor,
    )
    return result.reshape(1, columns, total_rows)


def solution(mesh):
    return jax.shard_map(
        functools.partial(on_device, mesh.shape["rows"]),
        mesh=mesh,
        in_specs=(
            P("cols", "rows", None),
            P(None, "cols"),
            P(),
            P(),
            P("rows", None, None),
            P("rows", None, None),
        ),
        out_specs=P("cols", "rows", None),
        check_vma=False,
    )
```

```python
import functools

import jax
import jax.numpy as jnp
from jax import lax
from jax.experimental import pallas as pl
from jax.experimental.pallas import tpu as pltpu
from jax.sharding import PartitionSpec as P

BLOCK = 128
COLS = 6
PAIR = 2
PARTS = 2


def split(value):
    high = value.astype(jnp.bfloat16)
    low = (value - high.astype(jnp.float32)).astype(jnp.bfloat16)
    return high, low


def times_transposed(x, high, low):
    dims = (((1,), (1,)), ((), ()))
    x_high, x_low = split(x)
    dot = functools.partial(lax.dot_general, dimension_numbers=dims, preferred_element_type=jnp.float32)
    return dot(x_high, high) + (dot(x_low, high) + dot(x_high, low))


def kernel(
    n, fronts, blocks, chunk,
    rhs_hbm, pattern_hbm, fb_hbm, slot_hbm, inv_hbm, upd_hbm,
    out_ref,
    x, snd, rcv, back, pool, last, halves, inv, upd, wide, sep_rows, coef,
    pattern, fb, slot, front_of, place_of, src, sep,
    local_sem, out_send, out_recv, back_send, back_recv,
):
    me = lax.axis_index("rows")
    col = lax.axis_index("cols")
    slots = PAIR * n
    seps = blocks - 2 * fronts
    few = n <= 16

    def target(peer):
        return {"rows": peer, "cols": col}

    half = n // PARTS

    def offset(p):
        return PARTS * (p % half) + p // half

    def for_part(g, body):
        first = max(g * half, 1)
        if few:
            for p in sorted(range(first, (g + 1) * half), key=lambda p: abs(offset(p) - n // 2)):
                body(p)
        else:
            def step(p, carry):
                body(p)
                return carry
            lax.fori_loop(first, (g + 1) * half, step, 0)

    def ahead(p):
        return lax.rem(me + offset(p), n)

    def behind(p):
        return lax.rem(me + n - offset(p), n)

    def repeat(count, body, unroll=1):
        def step(i, carry):
            body(i)
            return carry
        lax.fori_loop(0, count, step, 0, unroll=unroll if few else 1)

    pieces = [
        (rhs_hbm, x), (pattern_hbm, pattern), (fb_hbm, fb), (slot_hbm, slot), (inv_hbm, inv), (upd_hbm, upd),
    ]
    loads = [pltpu.make_async_copy(a, b, local_sem.at[i]) for i, (a, b) in enumerate(pieces)]
    for i in (3, 2, 1, 0):
        loads[i].start()

    barrier = pltpu.get_barrier_semaphore()
    for g in range(PARTS):
        for_part(g, lambda p: pl.semaphore_signal(
            barrier, inc=1, device_id=target(ahead(p)), device_id_type=pl.DeviceIdType.MESH
        ))
    for i in (4, 5):
        loads[i].start()

    def total(count, term):
        if few:
            values = [term(i) for i in range(count)]
            while len(values) > 1:
                pairs = [a + b for a, b in zip(values[::2], values[1::2])]
                values = pairs + ([values[-1]] if len(values) % 2 else [])
            return values[0]
        return lax.fori_loop(0, count, lambda i, t: t + term(i), 0)

    loads[3].wait()

    def find_front(s):
        front_of[s] = jnp.minimum(total(fronts, lambda f: jnp.where(slot[f] == s, f, 0)), fronts - 1)

    repeat(slots, find_front, 2)
    for i in (2, 1, 0):
        loads[i].wait()

    def block_rows(b, first, count):
        mask = pattern[b].astype(jnp.float32)
        return x[pl.ds(first * blocks + b, count, stride=blocks), :] * mask

    def pack(p):
        d = ahead(p)
        for k in range(PAIR):
            f = front_of[PAIR * d + k]
            b0, b1 = fb[0, f], fb[1, f]
            snd[k, p, 0] = block_rows(b0, 0, 4)
            snd[k, p, 1, 0:2, :] = block_rows(b0, 4, 2)
            snd[k, p, 1, 2:4, :] = block_rows(b1, 0, 2)
            snd[k, p, 2] = block_rows(b1, 2, 4)

    repeat(n, pack, 2)
    pl.semaphore_wait(barrier, n - 1)

    steps = [(k, g) for k in range(PAIR) for g in range(PARTS)]
    for i, (k, g) in enumerate(steps):
        for_part(g, lambda p, i=i, k=k: pltpu.make_async_remote_copy(
            src_ref=snd.at[k, p], dst_ref=rcv.at[k, p], send_sem=out_send.at[i], recv_sem=out_recv.at[i],
            device_id=target(ahead(p)), device_id_type=pl.DeviceIdType.MESH,
        ).start())
    for k in range(PAIR):
        rcv[k, 0] = snd[k, 0]

    loads[4].wait()
    loads[5].wait()
    width = inv.shape[1]
    strict = lax.broadcasted_iota(jnp.int32, (width, width), 0) > lax.broadcasted_iota(jnp.int32, (width, width), 1)
    for k in range(PAIR):
        wide[k, 0], wide[k, 1] = split(jnp.where(strict, inv[k], 0.0))
        wide[k, 2], wide[k, 3] = split(upd[k])
    halves[...] = jnp.zeros(halves.shape, jnp.float32)
    last[...] = jnp.zeros(last.shape, jnp.float32)

    def find_place(f):
        s = slot[f]
        away = lax.rem(lax.div(s, PAIR) + n - me, n)
        p = lax.rem(away, PARTS) * half + lax.div(away, PARTS)
        place_of[f] = 3 * (lax.rem(s, PAIR) * n + p) + 1

    repeat(fronts, find_place, 4)

    def find_source(b, rank):
        def term(f):
            at = place_of[f]
            return jnp.where(fb[0, f] == b, at, 0) + jnp.where(fb[1, f] == b, at + 1, 0)

        place = total(fronts, term)
        is_sep = place == 0
        src[b] = jnp.minimum(jnp.where(is_sep, 3 * slots + rank, place - 1), 3 * slots + seps - 1)
        return rank + jnp.where(is_sep, 1, 0)

    lax.fori_loop(0, blocks, find_source, 0)

    def landed(buffer, count, sem):
        view = buffer.at[pl.ds(0, count)]
        return pltpu.make_async_copy(view, view, sem)

    def flat(a):
        return a.reshape(8 * half, BLOCK)

    def remote(g):
        return half - 1 if g == 0 else half

    for i, (k, g) in enumerate(steps):
        landed(rcv.at[k], remote(g), out_recv.at[i]).wait()
        here = slice(g * half, (g + 1) * half)
        halves[i, 0, :, 0:4, :] = rcv[k, here, 0]
        halves[i, 0, :, 4:6, :] = rcv[k, here, 1, 0:2, :]
        halves[i, 1, :, 0:2, :] = rcv[k, here, 1, 2:4, :]
        halves[i, 1, :, 2:6, :] = rcv[k, here, 2]
        pivots = jnp.concatenate([flat(halves[i, 0]), flat(halves[i, 1])], axis=1)
        solved = pivots + times_transposed(pivots, wide[k, 0], wide[k, 1])
        update = times_transposed(solved, wide[k, 2], wide[k, 3])
        quads = [
            part.reshape(half, 8, BLOCK)
            for part in (solved[:, :BLOCK], solved[:, BLOCK:], update[:, :BLOCK], update[:, BLOCK:])
        ]
        for t in range(3):
            back[k, here, t, 0:6, :] = quads[t][:, 0:6]
            back[k, here, t, 6:8, :] = quads[3][:, 2 * t:2 * t + 2]

        for_part(g, lambda p, i=i, k=k: pltpu.make_async_remote_copy(
            src_ref=back.at[k, p], dst_ref=pool.at[pl.ds(3 * (k * n + p), 3)],
            send_sem=back_send.at[i], recv_sem=back_recv.at[i],
            device_id=target(behind(p)), device_id_type=pl.DeviceIdType.MESH,
        ).start())
        if g == 0:
            pool[3 * k * n:3 * k * n + 3] = back[k, 0]

    def find_separator(j):
        b = lax.fori_loop(
            0, blocks, lambda b, t: t + jnp.where(src[b] == 3 * slots + j, b, 0), 0, unroll=16 if few else 1
        )
        b = jnp.minimum(b, blocks - 1)
        sep[j] = b
        sep_rows[pl.ds(j, 1), :] = jnp.full((1, BLOCK), b, jnp.int32)
        pool[3 * slots + j, 0:6, :] = block_rows(b, 0, COLS)
        pool[3 * slots + j, 6:8, :] = jnp.zeros((2, BLOCK), jnp.float32)

    repeat(seps, find_separator)

    def weigh(g):
        rows = sep_rows[pl.ds(pl.multiple_of(g * chunk, chunk), chunk), :]

        def one_place(p):
            for k in range(PAIR):
                s = PAIR * ahead(p) + k
                f = front_of[s]
                used = slot[f] == s
                for h in range(2):
                    named = jnp.where(used, fb[2 + h, f], -1)
                    coef[(g * slots + k * n + p) * 2 + h] = jnp.where(rows == named, -1.0, 0.0)

        repeat(n, one_place, 4)

    repeat(seps // chunk, weigh)

    for i, (k, part) in enumerate(steps):
        landed(pool, 3 * remote(part), back_recv.at[i]).wait()
        begin = k * n + part * half
        for t in range(3):
            last[begin:begin + half, 2 * t:2 * t + 2, :] = pool[pl.ds(3 * begin + t, half, stride=3), 6:8, :]

        def add_up(g, begin=begin):
            first = 3 * slots + g * chunk

            def one_slot(o, accs):
                q = begin + o
                parts = (pool[3 * q + 2], last[q])
                for h in range(2):
                    row = (g * slots + q) * 2 + h
                    accs = tuple(a + coef[row, j:j + 1, :] * parts[h] for j, a in enumerate(accs))
                return accs

            accs = tuple(pool[first + j] for j in range(chunk))
            accs = lax.fori_loop(0, half, one_slot, accs, unroll=4 if few else 1)
            for j in range(chunk):
                pool[first + j] = accs[j]

        repeat(seps // chunk, add_up)

    def put(b):
        out_ref[pl.ds(b, COLS, stride=blocks), :] = pool[src[b], 0:6, :]

    repeat(blocks, put, 16)

    for i, (k, g) in enumerate(steps):
        landed(snd.at[k], remote(g), out_send.at[i]).wait()
        landed(back.at[k], remote(g), back_send.at[i]).wait()


def on_device(n, rhs, pattern, front_blocks, front_slot, pivot_inverse, update_factor):
    fronts = front_blocks.shape[0]
    columns, total_rows = rhs.shape[1:]
    blocks = total_rows // BLOCK
    assert columns == COLS and pivot_inverse.shape[0] == PAIR
    width = pivot_inverse.shape[1]
    slots = PAIR * n
    seps = blocks - 2 * fronts
    f32, i32 = jnp.float32, jnp.int32
    chunk = next(c for c in (16, 8, 4, 2, 1) if seps % c == 0)
    result = pl.pallas_call(
        functools.partial(kernel, n, fronts, blocks, chunk),
        out_shape=pltpu.VMEM((columns * blocks, BLOCK), f32),
        in_specs=[pl.BlockSpec(memory_space=pl.ANY)] * 6,
        out_specs=pl.BlockSpec(memory_space=pltpu.VMEM),
        scratch_shapes=[
            pltpu.VMEM((columns * blocks, BLOCK), f32),
            pltpu.VMEM((PAIR, n, 3, 4, BLOCK), f32),
            pltpu.VMEM((PAIR, n, 3, 4, BLOCK), f32),
            pltpu.VMEM((PAIR, n, 3, 8, BLOCK), f32),
            pltpu.VMEM((3 * slots + seps, 8, BLOCK), f32),
            pltpu.VMEM((slots, 8, BLOCK), f32),
            pltpu.VMEM((PAIR * PARTS, 2, n // PARTS, 8, BLOCK), f32),
            pltpu.VMEM((PAIR, width, width), f32),
            pltpu.VMEM((PAIR, width, width), f32),
            pltpu.VMEM((PAIR, 4, width, width), jnp.bfloat16),
            pltpu.VMEM((seps, BLOCK), i32),
            pltpu.VMEM((seps // chunk * slots * 2, chunk, BLOCK), f32),
            pltpu.SMEM((blocks,), i32),
            pltpu.SMEM((4, fronts), i32),
            pltpu.SMEM((fronts,), i32),
            pltpu.SMEM((slots,), i32),
            pltpu.SMEM((fronts,), i32),
            pltpu.SMEM((blocks,), i32),
            pltpu.SMEM((seps,), i32),
            pltpu.SemaphoreType.DMA((6,)),
            pltpu.SemaphoreType.DMA((PAIR * PARTS,)),
            pltpu.SemaphoreType.DMA((PAIR * PARTS,)),
            pltpu.SemaphoreType.DMA((PAIR * PARTS,)),
            pltpu.SemaphoreType.DMA((PAIR * PARTS,)),
        ],
        compiler_params=pltpu.CompilerParams(collective_id=0, has_side_effects=True),
    )(
        rhs.reshape(columns * blocks, BLOCK),
        pattern.reshape(-1),
        front_blocks.T,
        front_slot,
        pivot_inverse,
        update_factor,
    )
    return result.reshape(1, columns, total_rows)


def solution(mesh):
    return jax.shard_map(
        functools.partial(on_device, mesh.shape["rows"]),
        mesh=mesh,
        in_specs=(
            P("cols", "rows", None),
            P(None, "cols"),
            P(),
            P(),
            P("rows", None, None),
            P("rows", None, None),
        ),
        out_specs=P("cols", "rows", None),
        check_vma=False,
    )
```

```python
import functools

import jax
import jax.numpy as jnp
from jax import lax
from jax.experimental import pallas as pl
from jax.experimental.pallas import tpu as pltpu
from jax.sharding import PartitionSpec as P

BLOCK = 128
COLS = 6
PAIR = 2
PARTS = 4


def split(value):
    high = value.astype(jnp.bfloat16)
    low = (value - high.astype(jnp.float32)).astype(jnp.bfloat16)
    return high, low


def times_transposed(x, high, low):
    dims = (((1,), (1,)), ((), ()))
    x_high, x_low = split(x)
    dot = functools.partial(lax.dot_general, dimension_numbers=dims, preferred_element_type=jnp.float32)
    return dot(x_high, high) + (dot(x_low, high) + dot(x_high, low))


def kernel(
    n, fronts, blocks, chunk,
    rhs_hbm, pattern_hbm, fb_hbm, slot_hbm, inv_hbm, upd_hbm,
    out_ref,
    x, snd, rcv, back, pool, last, halves, inv, upd, wide, sep_rows, coef,
    pattern, fb, slot, front_of, place_of, src, sep,
    local_sem, out_send, out_recv, back_send, back_recv,
):
    me = lax.axis_index("rows")
    col = lax.axis_index("cols")
    slots = PAIR * n
    seps = blocks - 2 * fronts
    few = n <= 16

    def target(peer):
        return {"rows": peer, "cols": col}

    half = n // PARTS

    def offset(p):
        return PARTS * (p % half) + p // half

    def for_part(g, body):
        first = max(g * half, 1)
        if few:
            for p in sorted(range(first, (g + 1) * half), key=lambda p: abs(offset(p) - n // 2)):
                body(p)
        else:
            def step(p, carry):
                body(p)
                return carry
            lax.fori_loop(first, (g + 1) * half, step, 0)

    def ahead(p):
        return lax.rem(me + offset(p), n)

    def behind(p):
        return lax.rem(me + n - offset(p), n)

    def repeat(count, body, unroll=1):
        def step(i, carry):
            body(i)
            return carry
        lax.fori_loop(0, count, step, 0, unroll=unroll if few else 1)

    pieces = [
        (rhs_hbm, x), (pattern_hbm, pattern), (fb_hbm, fb), (slot_hbm, slot), (inv_hbm, inv), (upd_hbm, upd),
    ]
    loads = [pltpu.make_async_copy(a, b, local_sem.at[i]) for i, (a, b) in enumerate(pieces)]
    for i in (3, 2, 1, 0):
        loads[i].start()

    barrier = pltpu.get_barrier_semaphore()
    for g in range(PARTS):
        for_part(g, lambda p: pl.semaphore_signal(
            barrier, inc=1, device_id=target(ahead(p)), device_id_type=pl.DeviceIdType.MESH
        ))
    for i in (4, 5):
        loads[i].start()

    def total(count, term):
        if few:
            values = [term(i) for i in range(count)]
            while len(values) > 1:
                pairs = [a + b for a, b in zip(values[::2], values[1::2])]
                values = pairs + ([values[-1]] if len(values) % 2 else [])
            return values[0]
        return lax.fori_loop(0, count, lambda i, t: t + term(i), 0)

    loads[3].wait()

    def find_front(s):
        front_of[s] = jnp.minimum(total(fronts, lambda f: jnp.where(slot[f] == s, f, 0)), fronts - 1)

    repeat(slots, find_front, 2)
    for i in (2, 1, 0):
        loads[i].wait()

    def block_rows(b, first, count):
        mask = pattern[b].astype(jnp.float32)
        return x[pl.ds(first * blocks + b, count, stride=blocks), :] * mask

    def pack(p):
        d = ahead(p)
        for k in range(PAIR):
            f = front_of[PAIR * d + k]
            b0, b1 = fb[0, f], fb[1, f]
            snd[k, p, 0] = block_rows(b0, 0, 4)
            snd[k, p, 1, 0:2, :] = block_rows(b0, 4, 2)
            snd[k, p, 1, 2:4, :] = block_rows(b1, 0, 2)
            snd[k, p, 2] = block_rows(b1, 2, 4)

    repeat(n, pack, 2)
    pl.semaphore_wait(barrier, n - 1)

    steps = [(k, g) for k in range(PAIR) for g in range(PARTS)]
    for i, (k, g) in enumerate(steps):
        for_part(g, lambda p, i=i, k=k: pltpu.make_async_remote_copy(
            src_ref=snd.at[k, p], dst_ref=rcv.at[k, p], send_sem=out_send.at[i], recv_sem=out_recv.at[i],
            device_id=target(ahead(p)), device_id_type=pl.DeviceIdType.MESH,
        ).start())
    for k in range(PAIR):
        rcv[k, 0] = snd[k, 0]

    loads[4].wait()
    loads[5].wait()
    width = inv.shape[1]
    strict = lax.broadcasted_iota(jnp.int32, (width, width), 0) > lax.broadcasted_iota(jnp.int32, (width, width), 1)
    for k in range(PAIR):
        wide[k, 0], wide[k, 1] = split(jnp.where(strict, inv[k], 0.0))
        wide[k, 2], wide[k, 3] = split(upd[k])
    halves[...] = jnp.zeros(halves.shape, jnp.float32)
    last[...] = jnp.zeros(last.shape, jnp.float32)

    def find_place(f):
        s = slot[f]
        away = lax.rem(lax.div(s, PAIR) + n - me, n)
        p = lax.rem(away, PARTS) * half + lax.div(away, PARTS)
        place_of[f] = 3 * (lax.rem(s, PAIR) * n + p) + 1

    repeat(fronts, find_place, 4)

    def find_source(b, rank):
        def term(f):
            at = place_of[f]
            return jnp.where(fb[0, f] == b, at, 0) + jnp.where(fb[1, f] == b, at + 1, 0)

        place = total(fronts, term)
        is_sep = place == 0
        src[b] = jnp.minimum(jnp.where(is_sep, 3 * slots + rank, place - 1), 3 * slots + seps - 1)
        return rank + jnp.where(is_sep, 1, 0)

    lax.fori_loop(0, blocks, find_source, 0)

    def landed(buffer, count, sem):
        view = buffer.at[pl.ds(0, count)]
        return pltpu.make_async_copy(view, view, sem)

    def flat(a):
        return a.reshape(8 * half, BLOCK)

    def remote(g):
        return half - 1 if g == 0 else half

    for i, (k, g) in enumerate(steps):
        landed(rcv.at[k], remote(g), out_recv.at[i]).wait()
        here = slice(g * half, (g + 1) * half)
        halves[i, 0, :, 0:4, :] = rcv[k, here, 0]
        halves[i, 0, :, 4:6, :] = rcv[k, here, 1, 0:2, :]
        halves[i, 1, :, 0:2, :] = rcv[k, here, 1, 2:4, :]
        halves[i, 1, :, 2:6, :] = rcv[k, here, 2]
        pivots = jnp.concatenate([flat(halves[i, 0]), flat(halves[i, 1])], axis=1)
        solved = pivots + times_transposed(pivots, wide[k, 0], wide[k, 1])
        update = times_transposed(solved, wide[k, 2], wide[k, 3])
        quads = [
            part.reshape(half, 8, BLOCK)
            for part in (solved[:, :BLOCK], solved[:, BLOCK:], update[:, :BLOCK], update[:, BLOCK:])
        ]
        for t in range(3):
            back[k, here, t, 0:6, :] = quads[t][:, 0:6]
            back[k, here, t, 6:8, :] = quads[3][:, 2 * t:2 * t + 2]

        for_part(g, lambda p, i=i, k=k: pltpu.make_async_remote_copy(
            src_ref=back.at[k, p], dst_ref=pool.at[pl.ds(3 * (k * n + p), 3)],
            send_sem=back_send.at[i], recv_sem=back_recv.at[i],
            device_id=target(behind(p)), device_id_type=pl.DeviceIdType.MESH,
        ).start())
        if g == 0:
            pool[3 * k * n:3 * k * n + 3] = back[k, 0]

    def find_separator(j):
        b = lax.fori_loop(
            0, blocks, lambda b, t: t + jnp.where(src[b] == 3 * slots + j, b, 0), 0, unroll=16 if few else 1
        )
        b = jnp.minimum(b, blocks - 1)
        sep[j] = b
        sep_rows[pl.ds(j, 1), :] = jnp.full((1, BLOCK), b, jnp.int32)
        pool[3 * slots + j, 0:6, :] = block_rows(b, 0, COLS)
        pool[3 * slots + j, 6:8, :] = jnp.zeros((2, BLOCK), jnp.float32)

    repeat(seps, find_separator)

    def weigh(g):
        rows = sep_rows[pl.ds(pl.multiple_of(g * chunk, chunk), chunk), :]

        def one_place(p):
            for k in range(PAIR):
                s = PAIR * ahead(p) + k
                f = front_of[s]
                used = slot[f] == s
                for h in range(2):
                    named = jnp.where(used, fb[2 + h, f], -1)
                    coef[(g * slots + k * n + p) * 2 + h] = jnp.where(rows == named, -1.0, 0.0)

        repeat(n, one_place, 4)

    repeat(seps // chunk, weigh)

    for i, (k, part) in enumerate(steps):
        landed(pool, 3 * remote(part), back_recv.at[i]).wait()
        begin = k * n + part * half
        for t in range(3):
            last[begin:begin + half, 2 * t:2 * t + 2, :] = pool[pl.ds(3 * begin + t, half, stride=3), 6:8, :]

        def add_up(g, begin=begin):
            first = 3 * slots + g * chunk

            def one_slot(o, accs):
                q = begin + o
                parts = (pool[3 * q + 2], last[q])
                for h in range(2):
                    row = (g * slots + q) * 2 + h
                    accs = tuple(a + coef[row, j:j + 1, :] * parts[h] for j, a in enumerate(accs))
                return accs

            accs = tuple(pool[first + j] for j in range(chunk))
            accs = lax.fori_loop(0, half, one_slot, accs, unroll=4 if few else 1)
            for j in range(chunk):
                pool[first + j] = accs[j]

        repeat(seps // chunk, add_up)

    def put(b):
        out_ref[pl.ds(b, COLS, stride=blocks), :] = pool[src[b], 0:6, :]

    repeat(blocks, put, 16)

    for i, (k, g) in enumerate(steps):
        landed(snd.at[k], remote(g), out_send.at[i]).wait()
        landed(back.at[k], remote(g), back_send.at[i]).wait()


def on_device(n, rhs, pattern, front_blocks, front_slot, pivot_inverse, update_factor):
    fronts = front_blocks.shape[0]
    columns, total_rows = rhs.shape[1:]
    blocks = total_rows // BLOCK
    assert columns == COLS and pivot_inverse.shape[0] == PAIR
    width = pivot_inverse.shape[1]
    slots = PAIR * n
    seps = blocks - 2 * fronts
    f32, i32 = jnp.float32, jnp.int32
    chunk = next(c for c in (16, 8, 4, 2, 1) if seps % c == 0)
    result = pl.pallas_call(
        functools.partial(kernel, n, fronts, blocks, chunk),
        out_shape=pltpu.VMEM((columns * blocks, BLOCK), f32),
        in_specs=[pl.BlockSpec(memory_space=pl.ANY)] * 6,
        out_specs=pl.BlockSpec(memory_space=pltpu.VMEM),
        scratch_shapes=[
            pltpu.VMEM((columns * blocks, BLOCK), f32),
            pltpu.VMEM((PAIR, n, 3, 4, BLOCK), f32),
            pltpu.VMEM((PAIR, n, 3, 4, BLOCK), f32),
            pltpu.VMEM((PAIR, n, 3, 8, BLOCK), f32),
            pltpu.VMEM((3 * slots + seps, 8, BLOCK), f32),
            pltpu.VMEM((slots, 8, BLOCK), f32),
            pltpu.VMEM((PAIR * PARTS, 2, n // PARTS, 8, BLOCK), f32),
            pltpu.VMEM((PAIR, width, width), f32),
            pltpu.VMEM((PAIR, width, width), f32),
            pltpu.VMEM((PAIR, 4, width, width), jnp.bfloat16),
            pltpu.VMEM((seps, BLOCK), i32),
            pltpu.VMEM((seps // chunk * slots * 2, chunk, BLOCK), f32),
            pltpu.SMEM((blocks,), i32),
            pltpu.SMEM((4, fronts), i32),
            pltpu.SMEM((fronts,), i32),
            pltpu.SMEM((slots,), i32),
            pltpu.SMEM((fronts,), i32),
            pltpu.SMEM((blocks,), i32),
            pltpu.SMEM((seps,), i32),
            pltpu.SemaphoreType.DMA((6,)),
            pltpu.SemaphoreType.DMA((PAIR * PARTS,)),
            pltpu.SemaphoreType.DMA((PAIR * PARTS,)),
            pltpu.SemaphoreType.DMA((PAIR * PARTS,)),
            pltpu.SemaphoreType.DMA((PAIR * PARTS,)),
        ],
        compiler_params=pltpu.CompilerParams(collective_id=0, has_side_effects=True),
    )(
        rhs.reshape(columns * blocks, BLOCK),
        pattern.reshape(-1),
        front_blocks.T,
        front_slot,
        pivot_inverse,
        update_factor,
    )
    return result.reshape(1, columns, total_rows)


def solution(mesh):
    return jax.shard_map(
        functools.partial(on_device, mesh.shape["rows"]),
        mesh=mesh,
        in_specs=(
            P("cols", "rows", None),
            P(None, "cols"),
            P(),
            P(),
            P("rows", None, None),
            P("rows", None, None),
        ),
        out_specs=P("cols", "rows", None),
        check_vma=False,
    )
```

```python
import functools

import jax
import jax.numpy as jnp
from jax import lax
from jax.experimental import pallas as pl
from jax.experimental.pallas import tpu as pltpu
from jax.sharding import PartitionSpec as P

BLOCK = 128
COLS = 6
PAIR = 2
PARTS = 4


def split(value):
    high = value.astype(jnp.bfloat16)
    low = (value - high.astype(jnp.float32)).astype(jnp.bfloat16)
    return high, low


def times(x, high, low, inner):
    dims = (((1,), (inner,)), ((), ()))
    x_high, x_low = split(x)
    dot = functools.partial(lax.dot_general, dimension_numbers=dims, preferred_element_type=jnp.float32)
    return dot(x_high, high) + (dot(x_low, high) + dot(x_high, low))


def kernel(
    n, fronts, blocks, chunk,
    rhs_hbm, pattern_hbm, fb_hbm, slot_hbm, inv_hbm, upd_hbm,
    out_ref,
    x, snd, rcv, back, pool, last, halves, inv, upd, wide, sep_rows, coef,
    pattern, fb, slot, front_of, place_of, src, sep,
    local_sem, out_send, out_recv, back_send, back_recv,
):
    me = lax.axis_index("rows")
    col = lax.axis_index("cols")
    slots = PAIR * n
    seps = blocks - 2 * fronts
    few = n <= 16

    def target(peer):
        return {"rows": peer, "cols": col}

    half = n // PARTS

    def offset(p):
        return PARTS * (p % half) + p // half

    def for_part(g, body):
        first = max(g * half, 1)
        if few:
            for p in sorted(range(first, (g + 1) * half), key=lambda p: -abs(offset(p) - n // 2)):
                body(p)
        else:
            def step(p, carry):
                body(p)
                return carry
            lax.fori_loop(first, (g + 1) * half, step, 0)

    def ahead(p):
        return lax.rem(me + offset(p), n)

    def behind(p):
        return lax.rem(me + n - offset(p), n)

    def repeat(count, body, unroll=1):
        def step(i, carry):
            body(i)
            return carry
        lax.fori_loop(0, count, step, 0, unroll=unroll if few else 1)

    pieces = [
        (rhs_hbm, x), (pattern_hbm, pattern), (fb_hbm, fb), (slot_hbm, slot), (inv_hbm, inv), (upd_hbm, upd),
    ]
    loads = [pltpu.make_async_copy(a, b, local_sem.at[i]) for i, (a, b) in enumerate(pieces)]
    for i in (3, 2, 1, 0):
        loads[i].start()

    barrier = pltpu.get_barrier_semaphore()
    for g in range(PARTS):
        for_part(g, lambda p: pl.semaphore_signal(
            barrier, inc=1, device_id=target(ahead(p)), device_id_type=pl.DeviceIdType.MESH
        ))
    for i in (4, 5):
        loads[i].start()

    def total(count, term):
        if few:
            values = [term(i) for i in range(count)]
            while len(values) > 1:
                pairs = [a + b for a, b in zip(values[::2], values[1::2])]
                values = pairs + ([values[-1]] if len(values) % 2 else [])
            return values[0]
        return lax.fori_loop(0, count, lambda i, t: t + term(i), 0)

    loads[3].wait()

    def find_front(s):
        front_of[s] = jnp.minimum(total(fronts, lambda f: jnp.where(slot[f] == s, f, 0)), fronts - 1)

    repeat(slots, find_front, 2)
    for i in (2, 1, 0):
        loads[i].wait()

    def block_rows(b, first, count):
        mask = pattern[b].astype(jnp.float32)
        return x[pl.ds(first * blocks + b, count, stride=blocks), :] * mask

    def pack(p):
        d = ahead(p)
        for k in range(PAIR):
            f = front_of[PAIR * d + k]
            b0, b1 = fb[0, f], fb[1, f]
            snd[k, p, 0] = block_rows(b0, 0, 4)
            snd[k, p, 1, 0:2, :] = block_rows(b0, 4, 2)
            snd[k, p, 1, 2:4, :] = block_rows(b1, 0, 2)
            snd[k, p, 2] = block_rows(b1, 2, 4)

    repeat(n, pack, 2)
    pl.semaphore_wait(barrier, n - 1)

    steps = [(k, g) for k in range(PAIR) for g in range(PARTS)]
    for i, (k, g) in enumerate(steps):
        for_part(g, lambda p, i=i, k=k: pltpu.make_async_remote_copy(
            src_ref=snd.at[k, p], dst_ref=rcv.at[k, p], send_sem=out_send.at[i], recv_sem=out_recv.at[i],
            device_id=target(ahead(p)), device_id_type=pl.DeviceIdType.MESH,
        ).start())
    for k in range(PAIR):
        rcv[k, 0] = snd[k, 0]

    loads[4].wait()
    loads[5].wait()
    width = inv.shape[1]
    strict = lax.broadcasted_iota(jnp.int32, (width, width), 0) > lax.broadcasted_iota(jnp.int32, (width, width), 1)
    for k in range(PAIR):
        high, low = split(jnp.where(strict, inv[k], 0.0))
        wide[k, 0, :width], wide[k, 1, :width] = high, low
        wide[k, 0, width:], wide[k, 1, width:] = split(upd[k] + times(upd[k], high, low, 0))
    halves[...] = jnp.zeros(halves.shape, jnp.float32)
    last[...] = jnp.zeros(last.shape, jnp.float32)

    def find_place(f):
        s = slot[f]
        away = lax.rem(lax.div(s, PAIR) + n - me, n)
        p = lax.rem(away, PARTS) * half + lax.div(away, PARTS)
        place_of[f] = 3 * (lax.rem(s, PAIR) * n + p) + 1

    repeat(fronts, find_place, 4)

    def find_source(b, rank):
        def term(f):
            at = place_of[f]
            return jnp.where(fb[0, f] == b, at, 0) + jnp.where(fb[1, f] == b, at + 1, 0)

        place = total(fronts, term)
        is_sep = place == 0
        src[b] = jnp.minimum(jnp.where(is_sep, 3 * slots + rank, place - 1), 3 * slots + seps - 1)
        return rank + jnp.where(is_sep, 1, 0)

    lax.fori_loop(0, blocks, find_source, 0)

    def landed(buffer, count, sem):
        view = buffer.at[pl.ds(0, count)]
        return pltpu.make_async_copy(view, view, sem)

    def flat(a):
        return a.reshape(8 * half, BLOCK)

    def remote(g):
        return half - 1 if g == 0 else half

    for i, (k, g) in enumerate(steps):
        landed(rcv.at[k], remote(g), out_recv.at[i]).wait()
        here = slice(g * half, (g + 1) * half)
        halves[i, 0, :, 0:4, :] = rcv[k, here, 0]
        halves[i, 0, :, 4:6, :] = rcv[k, here, 1, 0:2, :]
        halves[i, 1, :, 0:2, :] = rcv[k, here, 1, 2:4, :]
        halves[i, 1, :, 2:6, :] = rcv[k, here, 2]
        pivots = jnp.concatenate([flat(halves[i, 0]), flat(halves[i, 1])], axis=1)
        both = times(pivots, wide[k, 0], wide[k, 1], 1)
        solved = pivots + both[:, :width]
        update = both[:, width:]
        quads = [
            part.reshape(half, 8, BLOCK)
            for part in (solved[:, :BLOCK], solved[:, BLOCK:], update[:, :BLOCK], update[:, BLOCK:])
        ]
        for t in range(3):
            back[k, here, t, 0:6, :] = quads[t][:, 0:6]
            back[k, here, t, 6:8, :] = quads[3][:, 2 * t:2 * t + 2]

        for_part(g, lambda p, i=i, k=k: pltpu.make_async_remote_copy(
            src_ref=back.at[k, p], dst_ref=pool.at[pl.ds(3 * (k * n + p), 3)],
            send_sem=back_send.at[i], recv_sem=back_recv.at[i],
            device_id=target(behind(p)), device_id_type=pl.DeviceIdType.MESH,
        ).start())
        if g == 0:
            pool[3 * k * n:3 * k * n + 3] = back[k, 0]

    def find_separator(j):
        b = lax.fori_loop(
            0, blocks, lambda b, t: t + jnp.where(src[b] == 3 * slots + j, b, 0), 0, unroll=16 if few else 1
        )
        b = jnp.minimum(b, blocks - 1)
        sep[j] = b
        sep_rows[pl.ds(j, 1), :] = jnp.full((1, BLOCK), b, jnp.int32)
        pool[3 * slots + j, 0:6, :] = block_rows(b, 0, COLS)
        pool[3 * slots + j, 6:8, :] = jnp.zeros((2, BLOCK), jnp.float32)

    repeat(seps, find_separator)

    def weigh(g):
        rows = sep_rows[pl.ds(pl.multiple_of(g * chunk, chunk), chunk), :]

        def one_place(p):
            for k in range(PAIR):
                s = PAIR * ahead(p) + k
                f = front_of[s]
                used = slot[f] == s
                for h in range(2):
                    named = jnp.where(used, fb[2 + h, f], -1)
                    coef[(g * slots + k * n + p) * 2 + h] = jnp.where(rows == named, -1.0, 0.0)

        repeat(n, one_place, 4)

    repeat(seps // chunk, weigh)

    for i, (k, part) in enumerate(steps):
        landed(pool, 3 * remote(part), back_recv.at[i]).wait()
        begin = k * n + part * half
        for t in range(3):
            last[begin:begin + half, 2 * t:2 * t + 2, :] = pool[pl.ds(3 * begin + t, half, stride=3), 6:8, :]

        def add_up(g, begin=begin):
            first = 3 * slots + g * chunk

            def one_slot(o, accs):
                q = begin + o
                parts = (pool[3 * q + 2], last[q])
                for h in range(2):
                    row = (g * slots + q) * 2 + h
                    accs = tuple(a + coef[row, j:j + 1, :] * parts[h] for j, a in enumerate(accs))
                return accs

            accs = tuple(pool[first + j] for j in range(chunk))
            accs = lax.fori_loop(0, half, one_slot, accs, unroll=4 if few else 1)
            for j in range(chunk):
                pool[first + j] = accs[j]

        repeat(seps // chunk, add_up)

    def put(b):
        out_ref[pl.ds(b, COLS, stride=blocks), :] = pool[src[b], 0:6, :]

    repeat(blocks, put, 16)

    for i, (k, g) in enumerate(steps):
        landed(snd.at[k], remote(g), out_send.at[i]).wait()
        landed(back.at[k], remote(g), back_send.at[i]).wait()


def on_device(n, rhs, pattern, front_blocks, front_slot, pivot_inverse, update_factor):
    fronts = front_blocks.shape[0]
    columns, total_rows = rhs.shape[1:]
    blocks = total_rows // BLOCK
    assert columns == COLS and pivot_inverse.shape[0] == PAIR
    width = pivot_inverse.shape[1]
    slots = PAIR * n
    seps = blocks - 2 * fronts
    f32, i32 = jnp.float32, jnp.int32
    chunk = next(c for c in (16, 8, 4, 2, 1) if seps % c == 0)
    result = pl.pallas_call(
        functools.partial(kernel, n, fronts, blocks, chunk),
        out_shape=pltpu.VMEM((columns * blocks, BLOCK), f32),
        in_specs=[pl.BlockSpec(memory_space=pl.ANY)] * 6,
        out_specs=pl.BlockSpec(memory_space=pltpu.VMEM),
        scratch_shapes=[
            pltpu.VMEM((columns * blocks, BLOCK), f32),
            pltpu.VMEM((PAIR, n, 3, 4, BLOCK), f32),
            pltpu.VMEM((PAIR, n, 3, 4, BLOCK), f32),
            pltpu.VMEM((PAIR, n, 3, 8, BLOCK), f32),
            pltpu.VMEM((3 * slots + seps, 8, BLOCK), f32),
            pltpu.VMEM((slots, 8, BLOCK), f32),
            pltpu.VMEM((PAIR * PARTS, 2, n // PARTS, 8, BLOCK), f32),
            pltpu.VMEM((PAIR, width, width), f32),
            pltpu.VMEM((PAIR, width, width), f32),
            pltpu.VMEM((PAIR, 2, 2 * width, width), jnp.bfloat16),
            pltpu.VMEM((seps, BLOCK), i32),
            pltpu.VMEM((seps // chunk * slots * 2, chunk, BLOCK), f32),
            pltpu.SMEM((blocks,), i32),
            pltpu.SMEM((4, fronts), i32),
            pltpu.SMEM((fronts,), i32),
            pltpu.SMEM((slots,), i32),
            pltpu.SMEM((fronts,), i32),
            pltpu.SMEM((blocks,), i32),
            pltpu.SMEM((seps,), i32),
            pltpu.SemaphoreType.DMA((6,)),
            pltpu.SemaphoreType.DMA((PAIR * PARTS,)),
            pltpu.SemaphoreType.DMA((PAIR * PARTS,)),
            pltpu.SemaphoreType.DMA((PAIR * PARTS,)),
            pltpu.SemaphoreType.DMA((PAIR * PARTS,)),
        ],
        compiler_params=pltpu.CompilerParams(collective_id=0, has_side_effects=True),
    )(
        rhs.reshape(columns * blocks, BLOCK),
        pattern.reshape(-1),
        front_blocks.T,
        front_slot,
        pivot_inverse,
        update_factor,
    )
    return result.reshape(1, columns, total_rows)


def solution(mesh):
    return jax.shard_map(
        functools.partial(on_device, mesh.shape["rows"]),
        mesh=mesh,
        in_specs=(
            P("cols", "rows", None),
            P(None, "cols"),
            P(),
            P(),
            P("rows", None, None),
            P("rows", None, None),
        ),
        out_specs=P("cols", "rows", None),
        check_vma=False,
    )
```

```python
import functools

import jax
import jax.numpy as jnp
from jax import lax
from jax.experimental import pallas as pl
from jax.experimental.pallas import tpu as pltpu
from jax.sharding import PartitionSpec as P

BLOCK = 128
COLS = 6
PAIR = 2
PARTS = 8


def split(value):
    high = value.astype(jnp.bfloat16)
    low = (value - high.astype(jnp.float32)).astype(jnp.bfloat16)
    return high, low


def times(x, high, low, inner):
    dims = (((1,), (inner,)), ((), ()))
    x_high, x_low = split(x)
    dot = functools.partial(lax.dot_general, dimension_numbers=dims, preferred_element_type=jnp.float32)
    return dot(x_high, high) + (dot(x_low, high) + dot(x_high, low))


def kernel(
    n, fronts, blocks, chunk,
    rhs_hbm, pattern_hbm, fb_hbm, slot_hbm, inv_hbm, upd_hbm,
    out_ref,
    x, snd, rcv, back, pool, last, halves, inv, upd, wide, sep_rows, coef,
    pattern, fb, slot, front_of, place_of, src, sep,
    local_sem, out_send, out_recv, back_send, back_recv,
):
    me = lax.axis_index("rows")
    col = lax.axis_index("cols")
    slots = PAIR * n
    seps = blocks - 2 * fronts
    few = n <= 16

    def target(peer):
        return {"rows": peer, "cols": col}

    half = n // PARTS

    def offset(p):
        return PARTS * (p % half) + p // half

    def for_part(g, body):
        first = max(g * half, 1)
        if few:
            for p in sorted(range(first, (g + 1) * half), key=lambda p: -abs(offset(p) - n // 2)):
                body(p)
        else:
            def step(p, carry):
                body(p)
                return carry
            lax.fori_loop(first, (g + 1) * half, step, 0)

    def ahead(p):
        return lax.rem(me + offset(p), n)

    def behind(p):
        return lax.rem(me + n - offset(p), n)

    def repeat(count, body, unroll=1):
        def step(i, carry):
            body(i)
            return carry
        lax.fori_loop(0, count, step, 0, unroll=unroll if few else 1)

    pieces = [
        (rhs_hbm, x), (pattern_hbm, pattern), (fb_hbm, fb), (slot_hbm, slot), (inv_hbm, inv), (upd_hbm, upd),
    ]
    loads = [pltpu.make_async_copy(a, b, local_sem.at[i]) for i, (a, b) in enumerate(pieces)]
    for i in (3, 2, 1, 0):
        loads[i].start()

    barrier = pltpu.get_barrier_semaphore()
    for g in range(PARTS):
        for_part(g, lambda p: pl.semaphore_signal(
            barrier, inc=1, device_id=target(ahead(p)), device_id_type=pl.DeviceIdType.MESH
        ))
    for i in (4, 5):
        loads[i].start()

    def total(count, term):
        if few:
            values = [term(i) for i in range(count)]
            while len(values) > 1:
                pairs = [a + b for a, b in zip(values[::2], values[1::2])]
                values = pairs + ([values[-1]] if len(values) % 2 else [])
            return values[0]
        return lax.fori_loop(0, count, lambda i, t: t + term(i), 0)

    loads[3].wait()

    def find_front(s):
        front_of[s] = jnp.minimum(total(fronts, lambda f: jnp.where(slot[f] == s, f, 0)), fronts - 1)

    repeat(slots, find_front, 2)
    for i in (2, 1, 0):
        loads[i].wait()

    def block_rows(b, first, count):
        mask = pattern[b].astype(jnp.float32)
        return x[pl.ds(first * blocks + b, count, stride=blocks), :] * mask

    def pack(p):
        d = ahead(p)
        for k in range(PAIR):
            f = front_of[PAIR * d + k]
            b0, b1 = fb[0, f], fb[1, f]
            snd[k, p, 0] = block_rows(b0, 0, 4)
            snd[k, p, 1, 0:2, :] = block_rows(b0, 4, 2)
            snd[k, p, 1, 2:4, :] = block_rows(b1, 0, 2)
            snd[k, p, 2] = block_rows(b1, 2, 4)

    repeat(n, pack, 2)
    pl.semaphore_wait(barrier, n - 1)

    steps = [(k, g) for g in range(PARTS) for k in range(PAIR)]
    for i, (k, g) in enumerate(steps):
        for_part(g, lambda p, i=i, k=k: pltpu.make_async_remote_copy(
            src_ref=snd.at[k, p], dst_ref=rcv.at[k, p], send_sem=out_send.at[i], recv_sem=out_recv.at[i],
            device_id=target(ahead(p)), device_id_type=pl.DeviceIdType.MESH,
        ).start())
    for k in range(PAIR):
        rcv[k, 0] = snd[k, 0]

    loads[4].wait()
    loads[5].wait()
    width = inv.shape[1]
    strict = lax.broadcasted_iota(jnp.int32, (width, width), 0) > lax.broadcasted_iota(jnp.int32, (width, width), 1)
    for k in range(PAIR):
        high, low = split(jnp.where(strict, inv[k], 0.0))
        wide[k, 0, :width], wide[k, 1, :width] = high, low
        wide[k, 0, width:], wide[k, 1, width:] = split(upd[k] + times(upd[k], high, low, 0))
    halves[...] = jnp.zeros(halves.shape, jnp.float32)
    last[...] = jnp.zeros(last.shape, jnp.float32)

    def find_place(f):
        s = slot[f]
        away = lax.rem(lax.div(s, PAIR) + n - me, n)
        p = lax.rem(away, PARTS) * half + lax.div(away, PARTS)
        place_of[f] = 3 * (lax.rem(s, PAIR) * n + p) + 1

    repeat(fronts, find_place, 4)

    def find_source(b, rank):
        def term(f):
            at = place_of[f]
            return jnp.where(fb[0, f] == b, at, 0) + jnp.where(fb[1, f] == b, at + 1, 0)

        place = total(fronts, term)
        is_sep = place == 0
        src[b] = jnp.minimum(jnp.where(is_sep, 3 * slots + rank, place - 1), 3 * slots + seps - 1)
        return rank + jnp.where(is_sep, 1, 0)

    lax.fori_loop(0, blocks, find_source, 0)

    def landed(buffer, count, sem):
        view = buffer.at[pl.ds(0, count)]
        return pltpu.make_async_copy(view, view, sem)

    def flat(a):
        return a.reshape(8 * half, BLOCK)

    def remote(g):
        return half - 1 if g == 0 else half

    for i, (k, g) in enumerate(steps):
        landed(rcv.at[k], remote(g), out_recv.at[i]).wait()
        here = slice(g * half, (g + 1) * half)
        halves[i, 0, :, 0:4, :] = rcv[k, here, 0]
        halves[i, 0, :, 4:6, :] = rcv[k, here, 1, 0:2, :]
        halves[i, 1, :, 0:2, :] = rcv[k, here, 1, 2:4, :]
        halves[i, 1, :, 2:6, :] = rcv[k, here, 2]
        pivots = jnp.concatenate([flat(halves[i, 0]), flat(halves[i, 1])], axis=1)
        both = times(pivots, wide[k, 0], wide[k, 1], 1)
        solved = pivots + both[:, :width]
        update = both[:, width:]
        quads = [
            part.reshape(half, 8, BLOCK)
            for part in (solved[:, :BLOCK], solved[:, BLOCK:], update[:, :BLOCK], update[:, BLOCK:])
        ]
        for t in range(3):
            back[k, here, t, 0:6, :] = quads[t][:, 0:6]
            back[k, here, t, 6:8, :] = quads[3][:, 2 * t:2 * t + 2]

        for_part(g, lambda p, i=i, k=k: pltpu.make_async_remote_copy(
            src_ref=back.at[k, p], dst_ref=pool.at[pl.ds(3 * (k * n + p), 3)],
            send_sem=back_send.at[i], recv_sem=back_recv.at[i],
            device_id=target(behind(p)), device_id_type=pl.DeviceIdType.MESH,
        ).start())
        if g == 0:
            pool[3 * k * n:3 * k * n + 3] = back[k, 0]

    def find_separator(j):
        b = lax.fori_loop(
            0, blocks, lambda b, t: t + jnp.where(src[b] == 3 * slots + j, b, 0), 0, unroll=16 if few else 1
        )
        b = jnp.minimum(b, blocks - 1)
        sep[j] = b
        sep_rows[pl.ds(j, 1), :] = jnp.full((1, BLOCK), b, jnp.int32)
        pool[3 * slots + j, 0:6, :] = block_rows(b, 0, COLS)
        pool[3 * slots + j, 6:8, :] = jnp.zeros((2, BLOCK), jnp.float32)

    repeat(seps, find_separator)

    def weigh(g):
        rows = sep_rows[pl.ds(pl.multiple_of(g * chunk, chunk), chunk), :]

        def one_place(p):
            for k in range(PAIR):
                s = PAIR * ahead(p) + k
                f = front_of[s]
                used = slot[f] == s
                for h in range(2):
                    named = jnp.where(used, fb[2 + h, f], -1)
                    coef[(g * slots + k * n + p) * 2 + h] = jnp.where(rows == named, -1.0, 0.0)

        repeat(n, one_place, 4)

    repeat(seps // chunk, weigh)

    for i, (k, part) in enumerate(steps):
        landed(pool, 3 * remote(part), back_recv.at[i]).wait()
        begin = k * n + part * half
        for t in range(3):
            last[begin:begin + half, 2 * t:2 * t + 2, :] = pool[pl.ds(3 * begin + t, half, stride=3), 6:8, :]

        def add_up(g, begin=begin):
            first = 3 * slots + g * chunk

            def one_slot(o, accs):
                q = begin + o
                parts = (pool[3 * q + 2], last[q])
                for h in range(2):
                    row = (g * slots + q) * 2 + h
                    accs = tuple(a + coef[row, j:j + 1, :] * parts[h] for j, a in enumerate(accs))
                return accs

            accs = tuple(pool[first + j] for j in range(chunk))
            accs = lax.fori_loop(0, half, one_slot, accs, unroll=4 if few else 1)
            for j in range(chunk):
                pool[first + j] = accs[j]

        repeat(seps // chunk, add_up)

    def put(b):
        out_ref[pl.ds(b, COLS, stride=blocks), :] = pool[src[b], 0:6, :]

    repeat(blocks, put, 16)

    for i, (k, g) in enumerate(steps):
        landed(snd.at[k], remote(g), out_send.at[i]).wait()
        landed(back.at[k], remote(g), back_send.at[i]).wait()


def on_device(n, rhs, pattern, front_blocks, front_slot, pivot_inverse, update_factor):
    fronts = front_blocks.shape[0]
    columns, total_rows = rhs.shape[1:]
    blocks = total_rows // BLOCK
    assert columns == COLS and pivot_inverse.shape[0] == PAIR
    width = pivot_inverse.shape[1]
    slots = PAIR * n
    seps = blocks - 2 * fronts
    f32, i32 = jnp.float32, jnp.int32
    chunk = next(c for c in (16, 8, 4, 2, 1) if seps % c == 0)
    result = pl.pallas_call(
        functools.partial(kernel, n, fronts, blocks, chunk),
        out_shape=pltpu.VMEM((columns * blocks, BLOCK), f32),
        in_specs=[pl.BlockSpec(memory_space=pl.ANY)] * 6,
        out_specs=pl.BlockSpec(memory_space=pltpu.VMEM),
        scratch_shapes=[
            pltpu.VMEM((columns * blocks, BLOCK), f32),
            pltpu.VMEM((PAIR, n, 3, 4, BLOCK), f32),
            pltpu.VMEM((PAIR, n, 3, 4, BLOCK), f32),
            pltpu.VMEM((PAIR, n, 3, 8, BLOCK), f32),
            pltpu.VMEM((3 * slots + seps, 8, BLOCK), f32),
            pltpu.VMEM((slots, 8, BLOCK), f32),
            pltpu.VMEM((PAIR * PARTS, 2, n // PARTS, 8, BLOCK), f32),
            pltpu.VMEM((PAIR, width, width), f32),
            pltpu.VMEM((PAIR, width, width), f32),
            pltpu.VMEM((PAIR, 2, 2 * width, width), jnp.bfloat16),
            pltpu.VMEM((seps, BLOCK), i32),
            pltpu.VMEM((seps // chunk * slots * 2, chunk, BLOCK), f32),
            pltpu.SMEM((blocks,), i32),
            pltpu.SMEM((4, fronts), i32),
            pltpu.SMEM((fronts,), i32),
            pltpu.SMEM((slots,), i32),
            pltpu.SMEM((fronts,), i32),
            pltpu.SMEM((blocks,), i32),
            pltpu.SMEM((seps,), i32),
            pltpu.SemaphoreType.DMA((6,)),
            pltpu.SemaphoreType.DMA((PAIR * PARTS,)),
            pltpu.SemaphoreType.DMA((PAIR * PARTS,)),
            pltpu.SemaphoreType.DMA((PAIR * PARTS,)),
            pltpu.SemaphoreType.DMA((PAIR * PARTS,)),
        ],
        compiler_params=pltpu.CompilerParams(collective_id=0, has_side_effects=True),
    )(
        rhs.reshape(columns * blocks, BLOCK),
        pattern.reshape(-1),
        front_blocks.T,
        front_slot,
        pivot_inverse,
        update_factor,
    )
    return result.reshape(1, columns, total_rows)


def solution(mesh):
    return jax.shard_map(
        functools.partial(on_device, mesh.shape["rows"]),
        mesh=mesh,
        in_specs=(
            P("cols", "rows", None),
            P(None, "cols"),
            P(),
            P(),
            P("rows", None, None),
            P("rows", None, None),
        ),
        out_specs=P("cols", "rows", None),
        check_vma=False,
    )
```
